512 devices in a mesh: row: 16 (over z), col: 32 (over y, x, core).
Axes of the slice: x: 4, y: 4, z: 16, core: 2. Of those that a mesh axis runs over, the one named last changes fastest.
Arguments:
- weight_basis: float32 [16384, 16384], P('row', 'col'), may hold values from -6 to 6
- panels: float32 [16384, 1024], P(('row', 'col')), may hold values from -1 to 1, as said below
- factors: float32 [256, 1024], P('col'), as said below
Outputs:
- rotated: float32 [16384, 16384], P('row', 'col')
The draws below stay inside these ranges and needn't reach their ends.
Inputs may be any that keep to these rules, and one draw needn't show every extreme that they name: Column k of panels is zero above row k and one at row k. Columns b * 256 to (b + 1) * 256 - 1 of factors hold an upper triangular T_b for which I - V_b T_b transpose(V_b) is orthogonal.
All inputs are finite; a program needn't handle non-finite values.
Results may differ from the reference program's by a relative error of at most 0.00012.
Values sent between devices are 32-bit elements; how exact they have to be, the bound alone decides.
No kernel may reach another device: no remote copies, remote signals or barrier semaphores. Data moves between devices by JAX's collectives and lax.ppermute only.
A program may use at most 64 MiB of HBM per device.

```python
import math
import jax
import jax.numpy as jnp
from jax import lax

N = 16384
TB = 256
NB = 4


def reflector_set(key):
    first = jax.random.fold_in(jax.random.fold_in(key, 17), 0)
    entries = jax.random.normal(first, (N, NB * TB), jnp.float32)
    row_index = lax.broadcasted_iota(jnp.int32, (N, NB * TB), 0)
    col_index = lax.broadcasted_iota(jnp.int32, (N, NB * TB), 1)
    below = entries / math.sqrt(N)
    return jnp.where(row_index > col_index, below, jnp.where(row_index == col_index, 1.0, 0.0)).astype(jnp.float32)


def draw_panels(key, part):
    return reflector_set(key)


def draw_factors(key, part):
    panels_all = reflector_set(key)
    pieces = []
    for index in range(NB):
        block = panels_all[:, index * TB:(index + 1) * TB]
        gram_block = jnp.dot(block.T, block, precision=lax.Precision.HIGHEST)
        inverse_form = jnp.triu(gram_block, 1) + jnp.diag(jnp.diag(gram_block)) * 0.5
        identity = jnp.eye(TB, dtype=jnp.float32)
        pieces.append(lax.linalg.triangular_solve(inverse_form, identity, left_side=True, lower=False))
    return jnp.concatenate(pieces, axis=1).astype(jnp.float32)


def shard_levels(stream_key, dims, cuts, least, largest):
    def one(axis_at, blocks):
        steps = jax.random.uniform(jax.random.fold_in(jax.random.fold_in(stream_key, 6), axis_at), (blocks,), jnp.float32, least / len(cuts), largest / len(cuts))
        return jnp.repeat(jnp.exp(steps), dims[axis_at] // blocks).reshape((-1,) + (1,) * (len(dims) - axis_at - 1))

    factor_of = one(*cuts[0])
    for cut in cuts[1:]:
        factor_of = factor_of * one(*cut)
    return factor_of


def scatter_about(own_key, shape, scale, most, cuts=(), held_as=jnp.bfloat16):
    array = jax.random.normal(own_key, shape, jnp.float32) * scale
    if len(cuts) > 0:
        array = shard_levels(own_key, shape, cuts, -0.22, 0.18) * array
    return jnp.clip(array, min=-most, max=most).astype(held_as)


def setup_inputs(seed: int = 0) -> dict:
    splits = jax.random.split(jax.random.key(seed), 4)
    return {
        "weight_basis": scatter_about(splits[0], (N, N), 1.0, 6.0, ((0, 16), (1, 32)), jnp.float32),
        "panels": draw_panels(jax.random.fold_in(splits[3], 71), 0),
        "factors": draw_factors(jax.random.fold_in(splits[3], 71), 0),
    }


def reference(weight_basis, panels, factors):
    exact = lax.Precision.HIGHEST
    current = weight_basis
    for block in reversed(range(NB)):
        vblock = panels[:, block * TB:(block + 1) * TB]
        triangle = factors[:, block * TB:(block + 1) * TB]
        projection = jnp.dot(vblock.T, current, precision=exact)
        applied = jnp.dot(triangle, projection, precision=exact)
        current = current - jnp.dot(vblock, applied, precision=exact)
    return current
```

```python
import jax
import jax.numpy as jnp
from jax import lax
from jax.sharding import PartitionSpec as P

HIGH = lax.Precision.HIGH
EXACT = lax.Precision.HIGHEST


def exchange_hops(ranks):
    hops, at = [], 1
    count = ranks.bit_length() - 1
    for step in range(count):
        hops.append(at)
        at += (-2) ** (step + 1)
    return hops


def block_order(ranks):
    hops = exchange_hops(ranks)

    def kept(rank, step):
        if step == len(hops):
            return [rank]
        hop = hops[step] if rank % 2 == 0 else -hops[step]
        return kept((rank + hop) % ranks, step + 1) + kept(rank, step + 1)

    return kept(0, 0)


def partners(rows, cols, hop):
    pairs = []
    for row in range(rows):
        for col in range(cols):
            sign = 1 if (row + col) % 2 == 0 else -1
            pairs.append((row * cols + col, (row + sign * hop) % rows * cols + col))
    return pairs


class Rows:
    def __init__(self, rows, cols):
        self.rows, self.cols = rows, cols
        self.pairs = [partners(rows, cols, hop) for hop in exchange_hops(rows)]
        order = block_order(rows)
        place = [order.index(block) for block in range(rows)]
        row, col = lax.axis_index("row"), lax.axis_index("col")
        sign = jnp.where((row + col) % 2 == 0, 1, -1)
        self.order = (row + sign * jnp.array(order, jnp.int32)) % rows
        self.place = jnp.array(place, jnp.int32)[sign * (jnp.arange(rows, dtype=jnp.int32) - row) % rows]

    def scattered(self, array):
        held = array.reshape(self.rows, -1, array.shape[1])[self.order]
        for pairs in self.pairs:
            half = held.shape[0] // 2
            held = held[half:] + lax.ppermute(held[:half], ("row", "col"), pairs)
        return held[0]

    def gathered(self, array):
        held = array[None]
        for pairs in reversed(self.pairs):
            held = jnp.concatenate([lax.ppermute(held, ("row", "col"), pairs), held])
        return held[self.place].reshape(-1, array.shape[1])


def gathered_halves(array, cols):
    height, width = array.shape
    halves = jnp.moveaxis(array.reshape(height, 2, width // 2), 1, 0)
    sent = jnp.broadcast_to(halves[None], (cols // 2, 2, height, width // 2)).reshape(cols, height, width // 2)
    own = lax.all_to_all(sent, "col", 0, 0, tiled=True).reshape(cols * height, width // 2)
    return own, lax.ppermute(own, "col", [(i, i ^ 1) for i in range(cols)])


def summed_over_rows(array, rows):
    height, width = array.shape
    tiles = -(-width // (128 * rows)) * rows
    padded = jnp.pad(array, ((0, 0), (0, tiles * 128 - width)))
    parts = jnp.moveaxis(padded.reshape(height, rows, -1), 1, 0)
    part = lax.all_to_all(parts, "row", 0, 0, tiled=True).sum(axis=0)
    sent = jnp.broadcast_to(part[None], parts.shape)
    whole = lax.all_to_all(sent, "row", 0, 0, tiled=True)
    return jnp.moveaxis(whole, 0, 1).reshape(height, -1)[:, :width]


def per_device(weight_basis, panels, factors):
    rows, cols = lax.axis_size("row"), lax.axis_size("col")
    over_rows = Rows(rows, cols)
    width = panels.shape[1]
    half = width // 2
    slab, block = factors.shape[0], factors.shape[0] * cols
    blocks = width // block
    col = lax.axis_index("col")
    first = col % 2 == 0

    def natural(own, other):
        return jnp.where(first, own, other), jnp.where(first, other, own)

    own, other = gathered_halves(panels, cols)

    def projected(v):
        w = lax.dot_general(weight_basis, v, (((0,), (0,)), ((), ())), precision=HIGH)
        return over_rows.scattered(w)

    w_own, w_other = projected(own), projected(other)

    picked = []
    for j in range(1, blocks):
        at = j * block % half + col * slab
        is_own = first == (j * block < half)
        a = lax.dynamic_slice(own, (0, at), (own.shape[0], slab))
        b = lax.dynamic_slice(other, (0, at), (own.shape[0], slab))
        picked.append(jnp.where(is_own, a, b))
    picked = jnp.concatenate(picked, axis=1)
    over = (((0,), (0,)), ((), ()))
    gram = jnp.concatenate(
        natural(
            lax.dot_general(picked, own, over, precision=EXACT),
            lax.dot_general(picked, other, over, precision=EXACT),
        ),
        axis=1,
    )
    gram = [gram[(j - 1) * slab : j * slab, : j * block] for j in range(1, blocks)]
    gram = summed_over_rows(jnp.concatenate(gram, axis=1), rows)
    small = jnp.concatenate(natural(*gathered_halves(jnp.concatenate([gram, factors], axis=1), cols)), axis=1)

    left = jnp.concatenate(natural(w_own, w_other), axis=1)
    applied, at = [], small.shape[1]
    for j in reversed(range(blocks)):
        triangle = small[:, at - block : at]
        at -= block
        applied.insert(
            0,
            lax.dot_general(left[:, j * block :], triangle, (((1,), (1,)), ((), ())), precision=EXACT),
        )
        if j:
            start = block * (j * (j - 1) // 2)
            cross = small[:, start : start + j * block]
            left = left[:, : j * block] - jnp.dot(applied[0], cross, precision=EXACT)
    applied = jnp.concatenate(applied, axis=1)
    y_own, y_other = natural(applied[:, :half], applied[:, half:])

    current = weight_basis
    for v, y in ((own, y_own), (other, y_other)):
        y = over_rows.gathered(y)
        current = current - lax.dot_general(v, y, (((1,), (1,)), ((), ())), precision=HIGH)
    return current


def solution(mesh):
    placed = (P("row", "col"), P(("row", "col"), None), P("col", None))
    return jax.shard_map(
        per_device, mesh=mesh, in_specs=placed, out_specs=P("row", "col"), check_vma=False
    )
```

```python
import functools

import jax
import jax.numpy as jnp
from jax import lax
from jax.experimental import pallas as pl
from jax.experimental.pallas import tpu as pltpu
from jax.sharding import PartitionSpec as P


EXACT = lax.Precision.HIGHEST


def exchange_hops(ranks):
    hops, at = [], 1
    count = ranks.bit_length() - 1
    for step in range(count):
        hops.append(at)
        at += (-2) ** (step + 1)
    return hops


def block_order(ranks):
    hops = exchange_hops(ranks)

    def kept(rank, step):
        if step == len(hops):
            return [rank]
        hop = hops[step] if rank % 2 == 0 else -hops[step]
        return kept((rank + hop) % ranks, step + 1) + kept(rank, step + 1)

    return kept(0, 0)


def partners(rows, cols, hop):
    pairs = []
    for row in range(rows):
        for col in range(cols):
            sign = 1 if (row + col) % 2 == 0 else -1
            pairs.append((row * cols + col, (row + sign * hop) % rows * cols + col))
    return pairs


class Rows:
    def __init__(self, rows, cols):
        self.pairs = [partners(rows, cols, hop) for hop in exchange_hops(rows)]
        row, col = lax.axis_index("row"), lax.axis_index("col")
        sign = jnp.where((row + col) % 2 == 0, 1, -1)
        self.order = (row + sign * jnp.array(block_order(rows), jnp.int32)) % rows

    def scattered(self, sent, kept):
        for pairs in self.pairs:
            come = lax.ppermute(sent, ("row", "col"), pairs)
            half = kept.shape[0] // 2
            if half == 0:
                return (kept + come)[0]
            sent = kept[:half] + come[:half]
            kept = kept[half:] + come[half:]

    def gathered(self, array):
        held = array[None]
        for pairs in reversed(self.pairs):
            come = lax.ppermute(held, ("row", "col"), pairs)
            if held.shape[0] * 2 == self.order.shape[0]:
                return come, held
            held = jnp.concatenate([come, held])


def parts_of(x):
    high = x.astype(jnp.bfloat16)
    return high, (x - high.astype(jnp.float32)).astype(jnp.bfloat16)


def product(a, b, dims):
    total = None
    for x, y in ((a[1], b[0]), (a[0], b[1]), (a[0], b[0])):
        term = lax.dot_general(x, y, dims, preferred_element_type=jnp.float32)
        total = term if total is None else total + term
    return total


def turned_kernel(c_ref, high_ref, low_ref):
    high_ref[...], low_ref[...] = parts_of(c_ref[...].T)


def turned(c):
    height, width = c.shape
    step = min(width, 128)
    out = jax.ShapeDtypeStruct((width, height), jnp.bfloat16)
    return pl.pallas_call(
        turned_kernel,
        grid=(width // step,),
        in_specs=[pl.BlockSpec((height, step), lambda i: (0, i))],
        out_specs=[pl.BlockSpec((step, height), lambda i: (i, 0))] * 2,
        out_shape=[out, out],
        cost_estimate=pl.CostEstimate(flops=8 * height * width, bytes_accessed=8 * height * width, transcendentals=0),
        name="turned",
    )(c)


def projection_kernel(step, order_ref, high_ref, low_ref, v_ref, sent_ref, kept_ref, w_ref, vhigh_ref, vlow_ref):
    vhigh_ref[...], vlow_ref[...] = parts_of(v_ref[...])
    v = vhigh_ref[...], vlow_ref[...]

    @pl.loop(0, w_ref.shape[0] // step)
    def _(i):
        at = pl.ds(pl.multiple_of(i * step, step), step)
        w_ref[at, :] = product((high_ref[at, :], low_ref[at, :]), v, (((1,), (0,)), ((), ())))

    half, size, _ = sent_ref.shape
    for i in range(2 * half):
        at = pl.ds(pl.multiple_of(order_ref[i] * size, size), size)
        if i < half:
            sent_ref[i] = w_ref[at, :]
        else:
            kept_ref[i - half] = w_ref[at, :]


def projection(order, c_parts, v):
    width, height = c_parts[0].shape
    ranks, rest = order.shape[0], v.shape[1]
    out = jax.ShapeDtypeStruct((ranks // 2, width // ranks, rest), jnp.float32)
    whole = pl.BlockSpec(memory_space=pltpu.VMEM)
    return pl.pallas_call(
        functools.partial(projection_kernel, min(width, 128)),
        in_specs=[pl.BlockSpec(memory_space=pltpu.SMEM), whole, whole, whole],
        out_specs=[whole, whole],
        out_shape=[out, out],
        scratch_shapes=[
            pltpu.VMEM((width, rest), jnp.float32),
            pltpu.VMEM((height, rest), jnp.bfloat16),
            pltpu.VMEM((height, rest), jnp.bfloat16),
        ],
        cost_estimate=pl.CostEstimate(
            flops=6 * width * height * rest, bytes_accessed=4 * (2 * width * rest + height * (width + rest)), transcendentals=0
        ),
        name="projection",
    )(order, *c_parts, v)


def update_kernel(step, order_ref, c_ref, v_ref, come_ref, held_ref, out_ref, high_ref, low_ref):
    half, size, _ = come_ref.shape
    for i in range(2 * half):
        at = pl.ds(pl.multiple_of(order_ref[i] * size, size), size)
        high_ref[at, :], low_ref[at, :] = parts_of(come_ref[i] if i < half else held_ref[i - half])
    y = high_ref[...], low_ref[...]

    @pl.loop(0, c_ref.shape[0] // step)
    def _(i):
        at = pl.ds(pl.multiple_of(i * step, step), step)
        out_ref[at, :] = c_ref[at, :] - product(parts_of(v_ref[at, :]), y, (((1,), (1,)), ((), ())))


def updated(order, c, v, come, held):
    height, width = c.shape
    rest = v.shape[1]
    whole = pl.BlockSpec(memory_space=pltpu.VMEM)
    return pl.pallas_call(
        functools.partial(update_kernel, min(height, 128)),
        in_specs=[pl.BlockSpec(memory_space=pltpu.SMEM), whole, whole, whole, whole],
        out_specs=whole,
        out_shape=jax.ShapeDtypeStruct((height, width), jnp.float32),
        scratch_shapes=[pltpu.VMEM((width, rest), jnp.bfloat16)] * 2,
        cost_estimate=pl.CostEstimate(
            flops=6 * width * height * rest, bytes_accessed=4 * (width * rest + height * (2 * width + rest)), transcendentals=0
        ),
        name="updated",
    )(order, c, v, come, held)


def gathered_halves(array, cols):
    height, width = array.shape
    halves = jnp.moveaxis(array.reshape(height, 2, width // 2), 1, 0)
    sent = jnp.broadcast_to(halves[None], (cols // 2, 2, height, width // 2)).reshape(cols, height, width // 2)
    own = lax.all_to_all(sent, "col", 0, 0, tiled=True).reshape(cols * height, width // 2)
    return own, lax.ppermute(own, "col", [(i, i ^ 1) for i in range(cols)])


def summed_over_rows(array, rows):
    height, width = array.shape
    tiles = -(-width // (128 * rows)) * rows
    padded = jnp.pad(array, ((0, 0), (0, tiles * 128 - width)))
    parts = jnp.moveaxis(padded.reshape(height, rows, -1), 1, 0)
    part = lax.all_to_all(parts, "row", 0, 0, tiled=True)
    sent = jnp.broadcast_to(part.sum(axis=0)[None], parts.shape)
    whole = lax.all_to_all(sent, "row", 0, 0, tiled=True)
    return jnp.moveaxis(whole, 0, 1).reshape(height, -1)[:, :width]


def per_device(weight_basis, panels, factors):
    rows, cols = lax.axis_size("row"), lax.axis_size("col")
    over_rows = Rows(rows, cols)
    width = panels.shape[1]
    half = width // 2
    slab, block = factors.shape[0], factors.shape[0] * cols
    blocks = width // block
    col = lax.axis_index("col")
    first = col % 2 == 0

    def natural(own, other):
        return jnp.where(first, own, other), jnp.where(first, other, own)

    own, other = gathered_halves(panels, cols)

    c_parts = turned(weight_basis)
    partial_own = projection(over_rows.order, c_parts, own)
    partial_other = projection(over_rows.order, c_parts, other)
    w_own = over_rows.scattered(*partial_own)
    w_other = over_rows.scattered(*partial_other)

    picked = []
    for j in range(1, blocks):
        at = j * block % half + col * slab
        is_own = first == (j * block < half)
        a = lax.dynamic_slice(own, (0, at), (own.shape[0], slab))
        b = lax.dynamic_slice(other, (0, at), (own.shape[0], slab))
        picked.append(jnp.where(is_own, a, b))
    picked = jnp.concatenate(picked, axis=1)
    over = (((0,), (0,)), ((), ()))
    gram = jnp.concatenate(
        natural(
            lax.dot_general(picked, own, over, precision=EXACT),
            lax.dot_general(picked, other, over, precision=EXACT),
        ),
        axis=1,
    )
    gram = [gram[(j - 1) * slab : j * slab, : j * block] for j in range(1, blocks)]
    gram = summed_over_rows(jnp.concatenate(gram, axis=1), rows)
    small = jnp.concatenate(natural(*gathered_halves(jnp.concatenate([gram, factors], axis=1), cols)), axis=1)

    left = jnp.concatenate(natural(w_own, w_other), axis=1)
    applied, at = [], small.shape[1]
    for j in reversed(range(blocks)):
        triangle = small[:, at - block : at]
        at -= block
        applied.insert(
            0,
            lax.dot_general(left[:, j * block :], triangle, (((1,), (1,)), ((), ())), precision=EXACT),
        )
        if j:
            start = block * (j * (j - 1) // 2)
            cross = small[:, start : start + j * block]
            left = left[:, : j * block] - jnp.dot(applied[0], cross, precision=EXACT)
    applied = jnp.concatenate(applied, axis=1)
    y_own, y_other = natural(applied[:, :half], applied[:, half:])

    current = weight_basis
    for v, y in ((own, y_own), (other, y_other)):
        current = updated(over_rows.order, current, v, *over_rows.gathered(y))
    return current


def solution(mesh):
    placed = (P("row", "col"), P(("row", "col"), None), P("col", None))
    return jax.shard_map(per_device, mesh=mesh, in_specs=placed, out_specs=P("row", "col"), check_vma=False)
```

```python
import jax
import jax.numpy as jnp
from jax import lax
from jax.experimental import pallas as pl
from jax.experimental.pallas import tpu as pltpu
from jax.sharding import PartitionSpec as P


EXACT = lax.Precision.HIGHEST


def exchange_hops(ranks):
    hops, at = [], 1
    count = ranks.bit_length() - 1
    for step in range(count):
        hops.append(at)
        at += (-2) ** (step + 1)
    return hops


def block_order(ranks):
    hops = exchange_hops(ranks)

    def kept(rank, step):
        if step == len(hops):
            return [rank]
        hop = hops[step] if rank % 2 == 0 else -hops[step]
        return kept((rank + hop) % ranks, step + 1) + kept(rank, step + 1)

    return kept(0, 0)


def partners(rows, cols, hop):
    pairs = []
    for row in range(rows):
        for col in range(cols):
            sign = 1 if (row + col) % 2 == 0 else -1
            pairs.append((row * cols + col, (row + sign * hop) % rows * cols + col))
    return pairs


class Rows:
    def __init__(self, rows, cols):
        self.pairs = [partners(rows, cols, hop) for hop in exchange_hops(rows)]
        row, col = lax.axis_index("row"), lax.axis_index("col")
        sign = jnp.where((row + col) % 2 == 0, 1, -1)
        self.order = (row + sign * jnp.array(block_order(rows), jnp.int32)) % rows

    def scattered(self, sent, kept):
        for pairs in self.pairs:
            come = lax.ppermute(sent, ("row", "col"), pairs)
            half = kept.shape[0] // 2
            if half == 0:
                return (kept + come)[0]
            sent = kept[:half] + come[:half]
            kept = kept[half:] + come[half:]

    def summed(self, array):
        for pairs in self.pairs:
            array = array + lax.ppermute(array, ("row", "col"), pairs)
        return array

    def gathered(self, array):
        held = array[None]
        for pairs in reversed(self.pairs):
            come = lax.ppermute(held, ("row", "col"), pairs)
            if held.shape[0] * 2 == self.order.shape[0]:
                return come, held
            held = jnp.concatenate([come, held])


def parts_of(x):
    high = x.astype(jnp.bfloat16)
    return high, (x - high.astype(jnp.float32)).astype(jnp.bfloat16)


def product(a, b, dims):
    total = None
    for x, y in ((a[1], b[0]), (a[0], b[1]), (a[0], b[0])):
        term = lax.dot_general(x, y, dims, preferred_element_type=jnp.float32)
        total = term if total is None else total + term
    return total


def turned_kernel(c_ref, high_ref, low_ref):
    high_ref[...], low_ref[...] = parts_of(c_ref[...].T)


def turned(c):
    height, width = c.shape
    step = min(width, 128)
    out = jax.ShapeDtypeStruct((width, height), jnp.bfloat16)
    return pl.pallas_call(
        turned_kernel,
        grid=(width // step,),
        in_specs=[pl.BlockSpec((height, step), lambda i: (0, i))],
        out_specs=[pl.BlockSpec((step, height), lambda i: (i, 0))] * 2,
        out_shape=[out, out],
        cost_estimate=pl.CostEstimate(flops=8 * height * width, bytes_accessed=8 * height * width, transcendentals=0),
        name="turned",
    )(c)


def projection_kernel(order_ref, high_ref, low_ref, v_ref, sent_ref, kept_ref, w_ref):
    w_ref[...] = product((high_ref[...], low_ref[...]), parts_of(v_ref[...]), (((1,), (0,)), ((), ())))
    half, size, _ = sent_ref.shape
    for i in range(2 * half):
        at = pl.ds(pl.multiple_of(order_ref[i] * size, size), size)
        if i < half:
            sent_ref[i] = w_ref[at, :]
        else:
            kept_ref[i - half] = w_ref[at, :]


def projection(order, c_parts, v):
    width, height = c_parts[0].shape
    ranks, rest = order.shape[0], v.shape[1]
    step = min(rest, 256)
    out = jax.ShapeDtypeStruct((ranks // 2, width // ranks, rest), jnp.float32)
    out_spec = pl.BlockSpec((ranks // 2, width // ranks, step), lambda i, order: (0, 0, i))
    c_spec = pl.BlockSpec((width, height), lambda i, order: (0, 0))
    return pl.pallas_call(
        projection_kernel,
        grid_spec=pltpu.PrefetchScalarGridSpec(
            num_scalar_prefetch=1,
            grid=(rest // step,),
            in_specs=[c_spec, c_spec, pl.BlockSpec((height, step), lambda i, order: (0, i))],
            out_specs=[out_spec, out_spec],
            scratch_shapes=[pltpu.VMEM((width, step), jnp.float32)],
        ),
        out_shape=[out, out],
        cost_estimate=pl.CostEstimate(
            flops=6 * width * height * rest, bytes_accessed=4 * (2 * width * rest + height * (width + rest)), transcendentals=0
        ),
        name="projection",
    )(order, *c_parts, v)


def update_kernel(order_ref, c_ref, v_ref, come_ref, held_ref, out_ref, placed_ref, high_ref, low_ref):
    @pl.when(pl.program_id(0) == 0)
    def _():
        half, size, _ = come_ref.shape
        for i in range(2 * half):
            at = pl.ds(pl.multiple_of(order_ref[i] * size, size), size)
            placed_ref[at, :] = come_ref[i] if i < half else held_ref[i - half]
        high_ref[...], low_ref[...] = parts_of(placed_ref[...].T)

    v, y = parts_of(v_ref[...]), (high_ref[...], low_ref[...])
    out_ref[...] = c_ref[...] - product(v, y, (((1,), (0,)), ((), ())))


def updated(order, c, v, come, held):
    height, width = c.shape
    rest = v.shape[1]
    step = min(height, 512)
    y_spec = pl.BlockSpec(come.shape, lambda i, order: (0, 0, 0))
    c_spec = pl.BlockSpec((step, width), lambda i, order: (i, 0))
    return pl.pallas_call(
        update_kernel,
        grid_spec=pltpu.PrefetchScalarGridSpec(
            num_scalar_prefetch=1,
            grid=(height // step,),
            in_specs=[c_spec, pl.BlockSpec((step, rest), lambda i, order: (i, 0)), y_spec, y_spec],
            out_specs=c_spec,
            scratch_shapes=[pltpu.VMEM((width, rest), jnp.float32)] + [pltpu.VMEM((rest, width), jnp.bfloat16)] * 2,
        ),
        out_shape=jax.ShapeDtypeStruct((height, width), jnp.float32),
        cost_estimate=pl.CostEstimate(
            flops=6 * width * height * rest, bytes_accessed=4 * (width * rest + height * (2 * width + rest)), transcendentals=0
        ),
        name="updated",
    )(order, c, v, come, held)


def gathered_halves(array, cols):
    height, width = array.shape
    halves = jnp.moveaxis(array.reshape(height, 2, width // 2), 1, 0)
    sent = jnp.broadcast_to(halves[None], (cols // 2, 2, height, width // 2)).reshape(cols, height, width // 2)
    own = lax.all_to_all(sent, "col", 0, 0, tiled=True).reshape(cols * height, width // 2)
    return own, lax.ppermute(own, "col", [(i, i ^ 1) for i in range(cols)])


def per_device(weight_basis, panels, factors):
    rows, cols = lax.axis_size("row"), lax.axis_size("col")
    over_rows = Rows(rows, cols)
    width = panels.shape[1]
    half = width // 2
    slab, block = factors.shape[0], factors.shape[0] * cols
    blocks = width // block
    col = lax.axis_index("col")
    first = col % 2 == 0

    def natural(own, other):
        return jnp.where(first, own, other), jnp.where(first, other, own)

    own, other = gathered_halves(panels, cols)

    c_parts = turned(weight_basis)
    partial_own = projection(over_rows.order, c_parts, own)
    partial_other = projection(over_rows.order, c_parts, other)
    w_own = over_rows.scattered(*partial_own)
    w_other = over_rows.scattered(*partial_other)

    picked = []
    for j in range(1, blocks):
        at = j * block % half + col * slab
        is_own = first == (j * block < half)
        a = lax.dynamic_slice(own, (0, at), (own.shape[0], slab))
        b = lax.dynamic_slice(other, (0, at), (own.shape[0], slab))
        picked.append(jnp.where(is_own, a, b))
    picked = jnp.concatenate(picked, axis=1)
    over = (((0,), (0,)), ((), ()))
    gram = jnp.concatenate(
        natural(
            lax.dot_general(picked, own, over, precision=EXACT),
            lax.dot_general(picked, other, over, precision=EXACT),
        ),
        axis=1,
    )
    gram = [gram[(j - 1) * slab : j * slab, : j * block] for j in range(1, blocks)]
    gram = over_rows.summed(jnp.concatenate(gram, axis=1))
    small = jnp.concatenate(natural(*gathered_halves(jnp.concatenate([gram, factors], axis=1), cols)), axis=1)

    left = jnp.concatenate(natural(w_own, w_other), axis=1)
    applied, at = [], small.shape[1]
    for j in reversed(range(blocks)):
        triangle = small[:, at - block : at]
        at -= block
        applied.insert(
            0,
            lax.dot_general(left[:, j * block :], triangle, (((1,), (1,)), ((), ())), precision=EXACT),
        )
        if j:
            start = block * (j * (j - 1) // 2)
            cross = small[:, start : start + j * block]
            left = left[:, : j * block] - jnp.dot(applied[0], cross, precision=EXACT)
    applied = jnp.concatenate(applied, axis=1)
    y_own, y_other = natural(applied[:, :half], applied[:, half:])

    current = weight_basis
    for v, y in ((own, y_own), (other, y_other)):
        current = updated(over_rows.order, current, v, *over_rows.gathered(y))
    return current


def solution(mesh):
    placed = (P("row", "col"), P(("row", "col"), None), P("col", None))
    return jax.shard_map(per_device, mesh=mesh, in_specs=placed, out_specs=P("row", "col"), check_vma=False)
```
